32 devices in a mesh: gx: 8 (over y, x, core), gy: 4 (over z).
Axes of the slice: x: 2, y: 2, z: 4, core: 2. Of those that a mesh axis runs over, the one named last changes fastest.
Arguments:
- terminal: float32 [128, 2048], P('gx', 'gy'), may hold values from -15 to 15
- initial_density: float32 [128, 2048], P('gx', 'gy'), may hold values from 0.1 to 1
- density_guess: float32 [2, 128, 2048], P(None, 'gx', 'gy'), may hold values from 0.1 to 1
- diagonal: float32 [128, 2048], P('gx', 'gy'), may hold values from 0.1 to 2
Outputs:
- value_field: float32 [128, 2048], P('gx', 'gy')
- density_field: float32 [128, 2048], P('gx', 'gy')
The draws below stay inside these ranges and needn't reach their ends.
All inputs are finite; a program needn't handle non-finite values.
Results may differ from the reference program's by a relative error of at most 0.00011.
Values sent between devices are 32-bit elements; how exact they have to be, the bound alone decides.
A program may use at most 64 MiB of HBM per device.

```python
import math
import jax
import jax.numpy as jnp

LEVELS = 2
STEPS = 3
NX = 128
NY = 2048


def draw_terminal(key, part):
    rows = jnp.arange(NX, dtype=jnp.float32)[:, None]
    scale = jnp.exp(jnp.log(3.0) * rows / max(NX - 1, 1))
    noise = jnp.clip(jax.random.normal(key, (NX, NY), jnp.float32), -5.0, 5.0)
    return scale * noise


def block_levels(rng, dims, pieces, low, largest):
    def one(position, shards_of):
        heights = jax.random.uniform(jax.random.fold_in(jax.random.fold_in(rng, 6), position), (shards_of,), jnp.float32, low / len(pieces), largest / len(pieces))
        return jnp.repeat(jnp.exp(heights), dims[position] // shards_of).reshape((-1,) + (1,) * (len(dims) - position - 1))

    gain = one(*pieces[0])
    for cut in pieces[1:]:
        gain = gain * one(*cut)
    return gain


def setup_inputs(seed: int = 0) -> dict:
    splits = jax.random.split(jax.random.key(seed), 5)
    terminal = draw_terminal(jax.random.fold_in(splits[4], 71), 0)
    initial_density = jnp.clip(jnp.exp(math.log(1.0) - 2.3025851 * jax.random.uniform(splits[1], (NX, NY), jnp.float32) ** block_levels(splits[1], (NX, NY), ((0, 8), (1, 4)), -0.2, 0.2)), 0.1, 1.0)
    density_guess = jnp.clip(jnp.exp(math.log(1.0) - 2.3025851 * jax.random.uniform(splits[2], (LEVELS, NX, NY), jnp.float32) ** block_levels(splits[2], (LEVELS, NX, NY), ((1, 8), (2, 4)), -0.2, 0.2)), 0.1, 1.0)
    diagonal = jnp.clip(jnp.exp(math.log(2.0) - 2.9957323 * jax.random.uniform(splits[3], (NX, NY), jnp.float32) ** block_levels(splits[3], (NX, NY), ((0, 8), (1, 4)), -0.2, 0.2)), 0.1, 2.0)
    return {"terminal": terminal, "initial_density": initial_density, "density_guess": density_guess, "diagonal": diagonal}


inv_step = 0.5
coupling = 0.5


def apply_padded(padded, center, diagonal):
    beside = padded[2:, 1:-1] + padded[:-2, 1:-1] + padded[1:-1, 2:] + padded[1:-1, :-2]
    return (inv_step + diagonal) * center + (4.0 * center - beside)


def hamiltonian(padded):
    center = padded[1:-1, 1:-1]
    back_x = center - padded[:-2, 1:-1]
    ahead_x = padded[2:, 1:-1] - center
    back_y = center - padded[1:-1, :-2]
    ahead_y = padded[1:-1, 2:] - center
    return 0.5 * (jnp.maximum(back_x, 0.0) ** 2 + jnp.minimum(ahead_x, 0.0) ** 2
                  + jnp.maximum(back_y, 0.0) ** 2 + jnp.minimum(ahead_y, 0.0) ** 2)


def divergence(pad_m, pad_u):
    m_mid = pad_m[1:-1, 1:-1]
    u_mid = pad_u[1:-1, 1:-1]
    speed_ahead = -(pad_u[2:, 1:-1] - u_mid)
    speed_back = -(u_mid - pad_u[:-2, 1:-1])
    flux_ahead = jnp.maximum(speed_ahead, 0.0) * m_mid + jnp.minimum(speed_ahead, 0.0) * pad_m[2:, 1:-1]
    flux_back = jnp.maximum(speed_back, 0.0) * pad_m[:-2, 1:-1] + jnp.minimum(speed_back, 0.0) * m_mid
    total = flux_ahead - flux_back
    speed_ahead = -(pad_u[1:-1, 2:] - u_mid)
    speed_back = -(u_mid - pad_u[1:-1, :-2])
    flux_ahead = jnp.maximum(speed_ahead, 0.0) * m_mid + jnp.minimum(speed_ahead, 0.0) * pad_m[1:-1, 2:]
    flux_back = jnp.maximum(speed_back, 0.0) * pad_m[1:-1, :-2] + jnp.minimum(speed_back, 0.0) * m_mid
    return total + flux_ahead - flux_back


def solve(rhs, diagonal):
    answer = jnp.zeros_like(rhs)
    resid = rhs
    direction = rhs
    norm_now = jnp.sum(resid * resid)
    for step in range(STEPS):
        image = apply_padded(jnp.pad(direction, 1), direction, diagonal)
        alpha = norm_now / jnp.sum(direction * image)
        answer = answer + alpha * direction
        resid = resid - alpha * image
        norm_next = jnp.sum(resid * resid)
        direction = resid + (norm_next / norm_now) * direction
        norm_now = norm_next
    return answer


def reference(terminal, initial_density, density_guess, diagonal):
    levels = [None] * LEVELS
    later = terminal
    for level in reversed(range(LEVELS)):
        rhs = inv_step * later - hamiltonian(jnp.pad(later, 1)) + coupling * density_guess[level]
        later = solve(rhs, diagonal)
        levels[level] = later
    density = initial_density
    for level in range(LEVELS):
        rhs = inv_step * density - divergence(jnp.pad(density, 1), jnp.pad(levels[level], 1))
        density = solve(rhs, diagonal)
    return levels[0], density
```

```python
import functools

import jax
import jax.numpy as jnp
from jax import lax
from jax.experimental import pallas as pl
from jax.experimental.pallas import tpu as pltpu
from jax.sharding import PartitionSpec as P

MESH = pl.DeviceIdType.MESH

LEVELS = 2
MARGIN = 16
LANES = 128

inv_step = 0.5
coupling = 0.5

SCALE = 0.2
SHIFT = 5.5

DIRECTIONS = [(r, c) for r in (-1, 0, 1) for c in (-1, 0, 1) if (r, c) != (0, 0)]
TINY = 2e-7


def solve_small(nu):
    g00 = nu[1] / SCALE + SHIFT * nu[0]
    g01 = nu[2] / SCALE + SHIFT * nu[1]
    g02 = nu[3] / SCALE + SHIFT * nu[2]
    g12 = nu[4] / SCALE + SHIFT * nu[3]
    g22 = nu[5] / SCALE + SHIFT * nu[4]
    g11 = g02
    inv0 = 1.0 / g00
    l10 = g01 * inv0
    l20 = g02 * inv0
    d1 = g11 - l10 * g01
    ok1 = d1 > TINY * g11
    inv1 = jnp.where(ok1, 1.0 / jnp.where(ok1, d1, 1.0), 0.0)
    t = g12 - l20 * g01
    l21 = t * inv1
    d2 = g22 - l20 * g02 - l21 * t
    ok2 = ok1 & (d2 > TINY * g22)
    inv2 = jnp.where(ok2, 1.0 / jnp.where(ok2, d2, 1.0), 0.0)
    y1 = nu[1] - l10 * nu[0]
    y2 = nu[2] - l20 * nu[0] - l21 * y1
    c2 = y2 * inv2
    c1 = y1 * inv1 - l21 * c2
    c0 = nu[0] * inv0 - l10 * c1 - l20 * c2
    return c0, c1, c2


def kernel(nx, ny, term_ref, dens_ref, guess_ref, diag_ref, value_ref, out_ref,
           main, left, right, sent, slots, halo_send, halo_recv, own_sem, sum_send, sum_recv):
    rows, cols = term_ref.shape
    gx = lax.axis_index("gx")
    gy = lax.axis_index("gy")
    count = nx * ny
    me = gx * ny + gy

    barrier = pltpu.get_barrier_semaphore()

    def partner(k):
        other = lax.rem(me + k, count)
        return (other // ny, lax.rem(other, ny))

    def greet(k, carry):
        pl.semaphore_signal(barrier, inc=1, device_id=partner(k), device_id_type=MESH)
        return carry

    lax.fori_loop(1, count, greet, 0)

    here = pl.ds(MARGIN, rows)
    own = [
        pltpu.make_async_copy(term_ref, main.at[0, here], own_sem.at[0]),
        pltpu.make_async_copy(guess_ref, main.at[pl.ds(3, 2), here], own_sem.at[1]),
        pltpu.make_async_copy(diag_ref, main.at[2, here], own_sem.at[2]),
        pltpu.make_async_copy(dens_ref, main.at[1, here], own_sem.at[3]),
    ]
    for copy in own:
        copy.start()
    pl.semaphore_wait(barrier, count - 1)

    def halo(d, a):
        dr, dc = DIRECTIONS[d]
        if dr == 0:
            src_rows, dst_rows = pl.ds(0, rows), pl.ds(MARGIN, rows)
        elif dr == 1:
            src_rows, dst_rows = pl.ds(rows - MARGIN, MARGIN), pl.ds(0, MARGIN)
        else:
            src_rows, dst_rows = pl.ds(0, MARGIN), pl.ds(MARGIN + rows, MARGIN)
        if dc == 0:
            src_cols, buf = pl.ds(0, cols), main
        elif dc == 1:
            src_cols, buf = pl.ds(cols - LANES, LANES), left
        else:
            src_cols, buf = pl.ds(0, LANES), right
        if a == 1:
            src = guess_ref.at[:, src_rows, src_cols]
            dst = buf.at[pl.ds(3, 2), dst_rows, :]
        else:
            ref, at = {0: (term_ref, 0), 2: (diag_ref, 2), 3: (dens_ref, 1)}[a]
            src = ref.at[src_rows, src_cols]
            dst = buf.at[at, dst_rows, :]
        return pltpu.make_async_remote_copy(
            src_ref=src, dst_ref=dst, send_sem=halo_send.at[d, a], recv_sem=halo_recv.at[d, a],
            device_id=(gx + dr, gy + dc), device_id_type=MESH)

    def inside(dr, dc):
        ok = None
        for here_at, step, size in ((gx, dr, nx), (gy, dc, ny)):
            if step == 1:
                test = here_at < size - 1
            elif step == -1:
                test = here_at > 0
            else:
                continue
            ok = test if ok is None else ok & test
        return ok

    for d, (dr, dc) in enumerate(DIRECTIONS):
        @pl.when(inside(dr, dc))
        def _():
            for a in range(4):
                halo(d, a).start()

    for copy in own:
        copy.wait()
    for d, (dr, dc) in enumerate(DIRECTIONS):
        @pl.when(inside(-dr, -dc))
        def _():
            for a in range(4):
                halo(d, a).wait_recv()

    tall, wide = rows + 2 * MARGIN, cols + LANES
    half = LANES // 2
    lane = lax.broadcasted_iota(jnp.int32, (tall, LANES), 1)

    def field(a):
        edge = jnp.where(lane < half, right[a], left[a])
        return jnp.concatenate([main[a], edge], axis=1)

    row = lax.broadcasted_iota(jnp.int32, (tall, wide), 0)
    col = lax.broadcasted_iota(jnp.int32, (tall, wide), 1)
    row_low = jnp.where(gx > 0, 0, MARGIN)
    row_high = jnp.where(gx < nx - 1, tall, MARGIN + rows)
    col_low = jnp.where(gy < ny - 1, cols + half, cols)
    col_high = jnp.where(gy > 0, cols + half, wide)
    mask = (row >= row_low) & (row < row_high) & ((col < col_low) | (col >= col_high))

    def masked(x):
        return jnp.where(mask, x, 0.0)

    def up(x):
        return pltpu.roll(x, 1, 0)

    def down(x):
        return pltpu.roll(x, x.shape[0] - 1, 0)

    def before(x):
        return pltpu.roll(x, 1, 1)

    def after(x):
        return pltpu.roll(x, x.shape[1] - 1, 1)

    core = SCALE * (field(2) + (inv_step + 4.0 - SHIFT))

    def apply_b(v):
        beside = (up(v) + down(v)) + (before(v) + after(v))
        return core * v - SCALE * beside

    def hamiltonian(u):
        dx = u - up(u)
        dy = u - before(u)
        px, qx = jnp.maximum(dx, 0.0), jnp.minimum(dx, 0.0)
        py, qy = jnp.maximum(dy, 0.0), jnp.minimum(dy, 0.0)
        return 0.5 * ((px * px + down(qx * qx)) + (py * py + after(qy * qy)))

    def faces(u):
        sx = u - down(u)
        sy = u - after(u)
        return jnp.maximum(sx, 0.0), jnp.minimum(sx, 0.0), jnp.maximum(sy, 0.0), jnp.minimum(sy, 0.0)

    def advance(m, face):
        px, qx, py, qy = face
        fx = px * m + qx * down(m)
        fy = py * m + qy * after(m)
        return masked(inv_step * m - ((fx - up(fx)) + (fy - before(fy))))

    def mine(x):
        return x[MARGIN:MARGIN + rows, :cols]

    def dot(x, y):
        return jnp.sum(x * y, keepdims=True)

    place = lax.broadcasted_iota(jnp.int32, (1, LANES), 1)

    def reduce(which, values):
        packed = jnp.zeros((1, LANES), jnp.float32)
        for k, value in enumerate(values):
            packed = jnp.where(place == k, value, packed)
        sent[which] = packed
        slots[which, me] = packed

        def send(k, carry):
            pltpu.make_async_remote_copy(
                src_ref=sent.at[which], dst_ref=slots.at[which, me],
                send_sem=sum_send.at[which], recv_sem=sum_recv.at[which],
                device_id=partner(k), device_id_type=MESH).start()
            return carry

        lax.fori_loop(1, count, send, 0)
        others = slots.at[which, pl.ds(0, count - 1)]
        pltpu.make_async_copy(others, others, sum_recv.at[which]).wait()
        total = jnp.sum(slots[which], axis=0)
        return [total[:, k:k + 1] for k in range(len(values))]

    def basis(b):
        v1 = masked(apply_b(b))
        v2 = masked(apply_b(v1))
        v3 = apply_b(v2)
        return b, v1, v2, v3

    def pairs(x, y):
        return [dot(x[0], y[0]), dot(x[0], y[1]), dot(x[1], y[1]),
                dot(x[1], y[2]), dot(x[2], y[2]), dot(x[2], y[3])]

    later = masked(field(0))
    values = [None, None]
    for level in (1, 0):
        b = masked(inv_step * later - hamiltonian(later) + coupling * field(3 + level))
        v = basis(b)
        w = [mine(x) for x in v]
        c = solve_small(reduce(1 - level, pairs(w, w)))
        later = c[0] * v[0] + c[1] * v[1] + c[2] * v[2]
        values[level] = later
    value_ref[...] = mine(values[0])

    density = masked(field(1))
    a = basis(advance(density, faces(values[0])))
    face = faces(values[1])
    inner = [mine(x) for x in a]
    families = [[mine(x) for x in basis(advance(a[i], face))] for i in range(3)]
    moments = pairs(inner, inner)
    for i in range(3):
        for j in range(i, 3):
            moments += pairs(families[i], families[j])
    total = reduce(2, moments)
    c = solve_small(total[:6])
    nu = [0.0] * 6
    at = 6
    for i in range(3):
        for j in range(i, 3):
            weight = c[i] * c[j] * (1.0 if i == j else 2.0)
            for k in range(6):
                nu[k] = nu[k] + weight * total[at + k]
            at += 6
    e = solve_small(nu)
    result = None
    for k in range(3):
        part = c[0] * families[0][k] + c[1] * families[1][k] + c[2] * families[2][k]
        result = e[k] * part if result is None else result + e[k] * part
    out_ref[...] = result

    for d, (dr, dc) in enumerate(DIRECTIONS):
        @pl.when(inside(dr, dc))
        def _():
            for a in range(4):
                halo(d, a).wait_send()
    for which in range(3):
        others = slots.at[which, pl.ds(0, count - 1)]
        pltpu.make_async_copy(others, others, sum_send.at[which]).wait()


def solution(mesh):
    nx, ny = mesh.shape["gx"], mesh.shape["gy"]

    def shards(terminal, initial_density, density_guess, diagonal):
        rows, cols = terminal.shape
        tall = rows + 2 * MARGIN
        hbm = pl.BlockSpec(memory_space=pl.ANY)
        vmem = pl.BlockSpec(memory_space=pltpu.VMEM)
        shape = jax.ShapeDtypeStruct((rows, cols), jnp.float32)
        return pl.pallas_call(
            functools.partial(kernel, nx, ny),
            out_shape=(shape, shape),
            in_specs=[hbm] * 4,
            out_specs=(vmem, vmem),
            scratch_shapes=[
                pltpu.VMEM((5, tall, cols), jnp.float32),
                pltpu.VMEM((5, tall, LANES), jnp.float32),
                pltpu.VMEM((5, tall, LANES), jnp.float32),
                pltpu.VMEM((3, 1, LANES), jnp.float32),
                pltpu.VMEM((3, nx * ny, 1, LANES), jnp.float32),
                pltpu.SemaphoreType.DMA((8, 4)),
                pltpu.SemaphoreType.DMA((8, 4)),
                pltpu.SemaphoreType.DMA((4,)),
                pltpu.SemaphoreType.DMA((3,)),
                pltpu.SemaphoreType.DMA((3,)),
            ],
            compiler_params=pltpu.CompilerParams(collective_id=0, has_side_effects=True),
        )(terminal, initial_density, density_guess, diagonal)

    placed = (P("gx", "gy"), P("gx", "gy"), P(None, "gx", "gy"), P("gx", "gy"))
    return jax.shard_map(
        shards,
        mesh=mesh,
        in_specs=placed,
        out_specs=(P("gx", "gy"), P("gx", "gy")),
        check_vma=False,
    )
```

```python
import functools

import jax
import jax.numpy as jnp
from jax import lax
from jax.experimental import pallas as pl
from jax.experimental.pallas import tpu as pltpu
from jax.sharding import PartitionSpec as P

MESH = pl.DeviceIdType.MESH

LEVELS = 2
MARGIN = 16
LANES = 128

inv_step = 0.5
coupling = 0.5

SCALE = 0.2
SHIFT = 5.5

DIRECTIONS = [(r, c) for r in (-1, 0, 1) for c in (-1, 0, 1) if (r, c) != (0, 0)]
TINY = 2e-7


def solve_small(nu):
    g00 = nu[1] / SCALE + SHIFT * nu[0]
    g01 = nu[2] / SCALE + SHIFT * nu[1]
    g02 = nu[3] / SCALE + SHIFT * nu[2]
    g12 = nu[4] / SCALE + SHIFT * nu[3]
    g22 = nu[5] / SCALE + SHIFT * nu[4]
    g11 = g02
    inv0 = 1.0 / g00
    l10 = g01 * inv0
    l20 = g02 * inv0
    d1 = g11 - l10 * g01
    ok1 = d1 > TINY * g11
    inv1 = jnp.where(ok1, 1.0 / jnp.where(ok1, d1, 1.0), 0.0)
    t = g12 - l20 * g01
    l21 = t * inv1
    d2 = g22 - l20 * g02 - l21 * t
    ok2 = ok1 & (d2 > TINY * g22)
    inv2 = jnp.where(ok2, 1.0 / jnp.where(ok2, d2, 1.0), 0.0)
    y1 = nu[1] - l10 * nu[0]
    y2 = nu[2] - l20 * nu[0] - l21 * y1
    c2 = y2 * inv2
    c1 = y1 * inv1 - l21 * c2
    c0 = nu[0] * inv0 - l10 * c1 - l20 * c2
    return c0, c1, c2


def kernel(nx, ny, term_ref, dens_ref, guess_ref, diag_ref, value_ref, out_ref,
           main, left, right, sent, slots, halo_send, halo_recv, own_sem, sum_send, sum_recv,
           ready):
    rows, cols = term_ref.shape
    gx = lax.axis_index("gx")
    gy = lax.axis_index("gy")
    count = nx * ny
    me = gx * ny + gy

    def inside(dr, dc):
        ok = None
        for here_at, step, size in ((gx, dr, nx), (gy, dc, ny)):
            if step == 1:
                test = here_at < size - 1
            elif step == -1:
                test = here_at > 0
            else:
                continue
            ok = test if ok is None else ok & test
        return ok

    def across(k):
        return (lax.rem(gx + k, nx), gy)

    def along(k):
        return (gx, lax.rem(gy + k, ny))

    barrier = pltpu.get_barrier_semaphore()
    greeted = nx + ny - 2
    for k in range(1, nx):
        pl.semaphore_signal(barrier, inc=1, device_id=across(k), device_id_type=MESH)
    for k in range(1, ny):
        pl.semaphore_signal(barrier, inc=1, device_id=along(k), device_id_type=MESH)
    for dr, dc in DIRECTIONS:
        if dr != 0 and dc != 0:
            there = inside(dr, dc)
            greeted = greeted + jnp.where(there, 1, 0)

            @pl.when(there)
            def _():
                pl.semaphore_signal(
                    barrier, inc=1, device_id=(gx + dr, gy + dc), device_id_type=MESH)

    here = pl.ds(MARGIN, rows)
    own = [
        pltpu.make_async_copy(source, main.at[at, here], own_sem.at[at])
        for at, source in enumerate(
            (term_ref, diag_ref, guess_ref.at[1], guess_ref.at[0], dens_ref))
    ]
    for copy in own:
        copy.start()
    for copy in own:
        copy.wait()
    pl.semaphore_wait(barrier, greeted)

    def pieces(dr):
        if dr == 0:
            return [(0, 3, 0, rows), (3, 2, 0, rows)]
        return [(0, 3, 0, 8), (0, 4, 8, 8), (3, 2, 0, 8)]

    def halo(d, piece):
        dr, dc = DIRECTIONS[d]
        first, many, out, size = pieces(dr)[piece]
        if dr == 0:
            src_rows, dst_rows = here, here
        elif dr == 1:
            src_rows = pl.ds(MARGIN + rows - out - size, size)
            dst_rows = pl.ds(MARGIN - out - size, size)
        else:
            src_rows = pl.ds(MARGIN + out, size)
            dst_rows = pl.ds(MARGIN + rows + out, size)
        if dc == 0:
            src_cols, buf = pl.ds(0, cols), main
        elif dc == 1:
            src_cols, buf = pl.ds(cols - LANES, LANES), left
        else:
            src_cols, buf = pl.ds(0, LANES), right
        return pltpu.make_async_remote_copy(
            src_ref=main.at[pl.ds(first, many), src_rows, src_cols],
            dst_ref=buf.at[pl.ds(first, many), dst_rows, :],
            send_sem=halo_send.at[d, piece], recv_sem=halo_recv.at[d, piece],
            device_id=(gx + dr, gy + dc), device_id_type=MESH)

    def each_halo(near, act, back=False):
        for d, (dr, dc) in enumerate(DIRECTIONS):
            @pl.when(inside(-dr, -dc) if back else inside(dr, dc))
            def _():
                for piece in [0] if near else range(1, len(pieces(dr))):
                    act(halo(d, piece))

    each_halo(True, lambda copy: copy.start())
    for k in range(1, nx):
        pl.semaphore_signal(ready, inc=1, device_id=across(k), device_id_type=MESH)
    each_halo(False, lambda copy: copy.start())

    wide = cols + LANES
    half = LANES // 2
    tall = rows + 2 * MARGIN
    low_mid, high_mid = MARGIN - 8, MARGIN + rows + 8

    def mask_of(size, cyclic, margin):
        row = lax.broadcasted_iota(jnp.int32, (size, wide), 0)
        col = lax.broadcasted_iota(jnp.int32, (size, wide), 1)
        col_low = jnp.where(gy < ny - 1, cols + half, cols)
        col_high = jnp.where(gy > 0, cols + half, wide)
        ok = (col < col_low) | (col >= col_high)
        if cyclic:
            row_low = jnp.where(gx < nx - 1, rows + 4, rows)
            row_high = jnp.where(gx > 0, rows + 4, size)
            return ok & ((row < row_low) | (row >= row_high))
        row_low = jnp.where(gx > 0, 0, margin)
        row_high = jnp.where(gx < nx - 1, size, margin + rows)
        return ok & (row >= row_low) & (row < row_high)

    masks = {
        "tall": mask_of(tall, False, MARGIN),
        "mid": mask_of(rows + 16, False, 8),
        "small": mask_of(rows + 8, True, 4),
    }

    def shrink(x, start):
        sub = lax.broadcasted_iota(jnp.int32, (8, x.shape[1]), 0)
        ends = jnp.where(sub < 4, x[start + rows:start + rows + 8], x[start - 8:start])
        return jnp.concatenate([x[start:start + rows], ends], axis=0)

    def strip(a, begin, end):
        lane = lax.broadcasted_iota(jnp.int32, (end - begin, LANES), 1)
        edge = jnp.where(lane < half, right[a, begin:end], left[a, begin:end])
        return jnp.concatenate([main[a, begin:end], edge], axis=1)

    def field(a, window):
        if window == "tall":
            return strip(a, 0, tall)
        x = strip(a, low_mid, high_mid)
        return x if window == "mid" else shrink(x, 8)

    def up(x):
        return pltpu.roll(x, 1, 0)

    def down(x):
        return pltpu.roll(x, x.shape[0] - 1, 0)

    def before(x):
        return pltpu.roll(x, 1, 1)

    def after(x):
        return pltpu.roll(x, x.shape[1] - 1, 1)

    def masked(x, window):
        return jnp.where(masks[window], x, 0.0)

    def core_of(window):
        return SCALE * (field(1, window) + (inv_step + 4.0 - SHIFT))

    def apply_b(v, core):
        beside = (up(v) + down(v)) + (before(v) + after(v))
        return core * v - SCALE * beside

    def hamiltonian(u):
        dx = u - up(u)
        dy = u - before(u)
        px, qx = jnp.maximum(dx, 0.0), jnp.minimum(dx, 0.0)
        py, qy = jnp.maximum(dy, 0.0), jnp.minimum(dy, 0.0)
        return 0.5 * ((px * px + down(qx * qx)) + (py * py + after(qy * qy)))

    def faces(u):
        sx = u - down(u)
        sy = u - after(u)
        return jnp.maximum(sx, 0.0), jnp.minimum(sx, 0.0), jnp.maximum(sy, 0.0), jnp.minimum(sy, 0.0)

    def advance(m, face, window):
        px, qx, py, qy = face
        fx = px * m + qx * down(m)
        fy = py * m + qy * after(m)
        return masked(inv_step * m - ((fx - up(fx)) + (fy - before(fy))), window)

    def value_rhs(later, level, window):
        return masked(inv_step * later - hamiltonian(later)
                      + coupling * field(2 if level == 1 else 3, window), window)

    def dot(x, y):
        return jnp.sum(x * y, keepdims=True)

    place = lax.broadcasted_iota(jnp.int32, (1, LANES), 1)

    def send_sums(which, values):
        packed = jnp.zeros((1, LANES), jnp.float32)
        for k, value in enumerate(values):
            packed = jnp.where(place == k, value, packed)
        sent[which] = packed
        slots[which, me] = packed

        def send(px, py):
            pltpu.make_async_remote_copy(
                src_ref=sent.at[which], dst_ref=slots.at[which, me],
                send_sem=sum_send.at[which], recv_sem=sum_recv.at[which],
                device_id=(px, py), device_id_type=MESH).start()

        columns = [lax.rem(gy + k, ny) for k in range(ny)]

        def line(k, carry):
            px = lax.rem(gx + k, nx)
            for py in columns:
                send(px, py)
            return carry

        lax.fori_loop(1, nx, line, 0)
        for py in columns[1:]:
            send(gx, py)

    def take_sums(which, many):
        others = slots.at[which, pl.ds(0, count - 1)]
        pltpu.make_async_copy(others, others, sum_recv.at[which]).wait()
        total = jnp.sum(slots[which], axis=0)
        return [total[:, k:k + 1] for k in range(many)]

    def basis(b, core, window, last=True):
        v1 = masked(apply_b(b, core), window)
        v2 = masked(apply_b(v1, core), window)
        return (b, v1, v2, apply_b(v2, core)) if last else (b, v1, v2)

    def mix(c, v):
        return c[0] * v[0] + c[1] * v[1] + c[2] * v[2]

    def pairs(x, y):
        return [dot(x[0], y[0]), dot(x[0], y[1]), dot(x[1], y[1]),
                dot(x[1], y[2]), dot(x[2], y[2]), dot(x[2], y[3])]

    def own_small(v):
        return [x[:rows, :cols] for x in v]

    each_halo(True, lambda copy: copy.wait_recv(), back=True)
    small_core = core_of("small")
    later = masked(field(0, "small"), "small")
    w = own_small(basis(value_rhs(later, 1, "small"), small_core, "small"))
    moments = pairs(w, w)
    pl.semaphore_wait(ready, nx - 1)
    send_sums(0, moments)
    each_halo(False, lambda copy: copy.wait_recv(), back=True)
    core = core_of("tall")
    later = masked(field(0, "tall"), "tall")
    v = basis(value_rhs(later, 1, "tall"), core, "tall", last=False)
    vs = [shrink(x, MARGIN) for x in v]
    c = solve_small(take_sums(0, 6))

    first_small = mix(c, vs)
    w = own_small(basis(value_rhs(first_small, 0, "small"), small_core, "small"))
    send_sums(1, pairs(w, w))
    first = mix(c, v)
    v = basis(value_rhs(first, 0, "tall"), core, "tall", last=False)
    v = [x[low_mid:high_mid] for x in v]
    face = faces(first_small)
    density = masked(field(4, "mid"), "mid")
    mid_core = core_of("mid")
    c = solve_small(take_sums(1, 6))
    second = mix(c, v)

    a = basis(advance(density, faces(second), "mid"), mid_core, "mid", last=False)
    a = [shrink(x, 8) for x in a]
    last = apply_b(a[2], small_core)
    inner = own_small(a + [last])
    families = [
        own_small(basis(advance(a[i], face, "small"), small_core, "small")) for i in range(3)]
    moments = pairs(inner, inner)
    for i in range(3):
        for j in range(i, 3):
            moments += pairs(families[i], families[j])
    send_sums(2, moments)
    value_ref[...] = second[8:8 + rows, :cols]
    total = take_sums(2, len(moments))
    c = solve_small(total[:6])
    nu = [0.0] * 6
    at = 6
    for i in range(3):
        for j in range(i, 3):
            weight = c[i] * c[j] * (1.0 if i == j else 2.0)
            for k in range(6):
                nu[k] = nu[k] + weight * total[at + k]
            at += 6
    e = solve_small(nu)
    result = None
    for i in range(3):
        for k in range(3):
            part = (c[i] * e[k]) * families[i][k]
            result = part if result is None else result + part
    out_ref[...] = result

    each_halo(True, lambda copy: copy.wait_send())
    each_halo(False, lambda copy: copy.wait_send())
    for which in range(3):
        others = slots.at[which, pl.ds(0, count - 1)]
        pltpu.make_async_copy(others, others, sum_send.at[which]).wait()


def deliver(value_ref, density_ref, value_out, density_out):
    value_out[...] = value_ref[...]
    density_out[...] = density_ref[...]


def solution(mesh):
    nx, ny = mesh.shape["gx"], mesh.shape["gy"]

    def shards(terminal, initial_density, density_guess, diagonal):
        rows, cols = terminal.shape
        tall = rows + 2 * MARGIN
        hbm = pl.BlockSpec(memory_space=pl.ANY)
        vmem = pl.BlockSpec(memory_space=pltpu.VMEM)
        shape = jax.ShapeDtypeStruct((rows, cols), jnp.float32)
        value, density = pl.pallas_call(
            functools.partial(kernel, nx, ny),
            out_shape=(shape, shape),
            in_specs=[hbm] * 4,
            out_specs=(vmem, vmem),
            scratch_shapes=[
                pltpu.VMEM((5, tall, cols), jnp.float32),
                pltpu.VMEM((5, tall, LANES), jnp.float32),
                pltpu.VMEM((5, tall, LANES), jnp.float32),
                pltpu.VMEM((3, 1, LANES), jnp.float32),
                pltpu.VMEM((3, nx * ny, 1, LANES), jnp.float32),
                pltpu.SemaphoreType.DMA((8, 3)),
                pltpu.SemaphoreType.DMA((8, 3)),
                pltpu.SemaphoreType.DMA((5,)),
                pltpu.SemaphoreType.DMA((3,)),
                pltpu.SemaphoreType.DMA((3,)),
                pltpu.SemaphoreType.REGULAR,
            ],
            compiler_params=pltpu.CompilerParams(collective_id=0, has_side_effects=True),
        )(terminal, initial_density, density_guess, diagonal)
        return pl.pallas_call(
            deliver,
            out_shape=(shape, shape),
            in_specs=[vmem] * 2,
            out_specs=(vmem, vmem),
        )(value, density)

    placed = (P("gx", "gy"), P("gx", "gy"), P(None, "gx", "gy"), P("gx", "gy"))
    return jax.shard_map(
        shards,
        mesh=mesh,
        in_specs=placed,
        out_specs=(P("gx", "gy"), P("gx", "gy")),
        check_vma=False,
    )
```

```python
import functools

import jax
import jax.numpy as jnp
from jax import lax
from jax.experimental import pallas as pl
from jax.experimental.pallas import tpu as pltpu
from jax.sharding import PartitionSpec as P

MESH = pl.DeviceIdType.MESH

LEVELS = 2
MARGIN = 16
LANES = 128

inv_step = 0.5
coupling = 0.5

SCALE = 0.25
SHIFT = 5.5

DIRECTIONS = [(r, c) for r in (-1, 0, 1) for c in (-1, 0, 1) if (r, c) != (0, 0)]
TINY = 2e-7


def solve_small(nu):
    g00 = nu[1] / SCALE + SHIFT * nu[0]
    g01 = nu[2] / SCALE + SHIFT * nu[1]
    g02 = nu[3] / SCALE + SHIFT * nu[2]
    g12 = nu[4] / SCALE + SHIFT * nu[3]
    g22 = nu[5] / SCALE + SHIFT * nu[4]
    g11 = g02
    inv0 = 1.0 / g00
    l10 = g01 * inv0
    l20 = g02 * inv0
    d1 = g11 - l10 * g01
    ok1 = d1 > TINY * g11
    inv1 = jnp.where(ok1, 1.0 / jnp.where(ok1, d1, 1.0), 0.0)
    t = g12 - l20 * g01
    l21 = t * inv1
    d2 = g22 - l20 * g02 - l21 * t
    ok2 = ok1 & (d2 > TINY * g22)
    inv2 = jnp.where(ok2, 1.0 / jnp.where(ok2, d2, 1.0), 0.0)
    y1 = nu[1] - l10 * nu[0]
    y2 = nu[2] - l20 * nu[0] - l21 * y1
    c2 = y2 * inv2
    c1 = y1 * inv1 - l21 * c2
    c0 = nu[0] * inv0 - l10 * c1 - l20 * c2
    return c0, c1, c2


def kernel(nx, ny, term_ref, dens_ref, guess_ref, diag_ref, both_ref,
           main, left, right, sent, slots, halo_send, halo_recv, own_sem, sum_send, sum_recv,
           ready, scaled_tall, scaled_mid, scaled_small):
    rows, cols = term_ref.shape
    gx = lax.axis_index("gx")
    gy = lax.axis_index("gy")
    count = nx * ny
    me = gx * ny + gy

    def inside(dr, dc):
        ok = None
        for here_at, step, size in ((gx, dr, nx), (gy, dc, ny)):
            if step == 1:
                test = here_at < size - 1
            elif step == -1:
                test = here_at > 0
            else:
                continue
            ok = test if ok is None else ok & test
        return ok

    def across(k):
        return (lax.rem(gx + k, nx), gy)

    def along(k):
        return (gx, lax.rem(gy + k, ny))

    barrier = pltpu.get_barrier_semaphore()
    greeted = nx + ny - 2
    for k in range(1, nx):
        pl.semaphore_signal(barrier, inc=1, device_id=across(k), device_id_type=MESH)
    for k in range(1, ny):
        pl.semaphore_signal(barrier, inc=1, device_id=along(k), device_id_type=MESH)
    for dr, dc in DIRECTIONS:
        if dr != 0 and dc != 0:
            there = inside(dr, dc)
            greeted = greeted + jnp.where(there, 1, 0)

            @pl.when(there)
            def _():
                pl.semaphore_signal(
                    barrier, inc=1, device_id=(gx + dr, gy + dc), device_id_type=MESH)

    here = pl.ds(MARGIN, rows)
    own = [
        pltpu.make_async_copy(source, main.at[at, here], own_sem.at[at])
        for at, source in enumerate(
            (term_ref, diag_ref, guess_ref.at[1], guess_ref.at[0], dens_ref))
    ]
    for copy in own:
        copy.start()
    wide = cols + LANES
    half = LANES // 2
    tall = rows + 2 * MARGIN
    low_mid, high_mid = MARGIN - 8, MARGIN + rows + 8

    def mask_of(size, cyclic, margin):
        row = lax.broadcasted_iota(jnp.int32, (size, wide), 0)
        col = lax.broadcasted_iota(jnp.int32, (size, wide), 1)
        col_low = jnp.where(gy < ny - 1, cols + half, cols)
        col_high = jnp.where(gy > 0, cols + half, wide)
        ok = (col < col_low) | (col >= col_high)
        if cyclic:
            row_low = jnp.where(gx < nx - 1, rows + 4, rows)
            row_high = jnp.where(gx > 0, rows + 4, size)
            return ok & ((row < row_low) | (row >= row_high))
        row_low = jnp.where(gx > 0, 0, margin)
        row_high = jnp.where(gx < nx - 1, size, margin + rows)
        return ok & (row >= row_low) & (row < row_high)

    scaled = {"tall": scaled_tall, "mid": scaled_mid, "small": scaled_small}
    scaled_tall[...] = jnp.where(mask_of(tall, False, MARGIN), SCALE, 0.0)
    scaled_mid[...] = jnp.where(mask_of(rows + 16, False, 8), SCALE, 0.0)
    scaled_small[...] = jnp.where(mask_of(rows + 8, True, 4), SCALE, 0.0)

    for copy in own:
        copy.wait()
    pl.semaphore_wait(barrier, greeted)

    def pieces(dr):
        if dr == 0:
            return [(0, 3, 0, rows), (3, 2, 0, rows)]
        return [(0, 3, 0, 8), (0, 4, 8, 8), (3, 2, 0, 8)]

    def halo(d, piece):
        dr, dc = DIRECTIONS[d]
        first, many, out, size = pieces(dr)[piece]
        if dr == 0:
            src_rows, dst_rows = here, here
        elif dr == 1:
            src_rows = pl.ds(MARGIN + rows - out - size, size)
            dst_rows = pl.ds(MARGIN - out - size, size)
        else:
            src_rows = pl.ds(MARGIN + out, size)
            dst_rows = pl.ds(MARGIN + rows + out, size)
        if dc == 0:
            src_cols, buf = pl.ds(0, cols), main
        elif dc == 1:
            src_cols, buf = pl.ds(cols - LANES, LANES), left
        else:
            src_cols, buf = pl.ds(0, LANES), right
        return pltpu.make_async_remote_copy(
            src_ref=main.at[pl.ds(first, many), src_rows, src_cols],
            dst_ref=buf.at[pl.ds(first, many), dst_rows, :],
            send_sem=halo_send.at[d, piece], recv_sem=halo_recv.at[d, piece],
            device_id=(gx + dr, gy + dc), device_id_type=MESH)

    def each_halo(near, act, back=False):
        for d, (dr, dc) in enumerate(DIRECTIONS):
            @pl.when(inside(-dr, -dc) if back else inside(dr, dc))
            def _():
                for piece in [0] if near else range(1, len(pieces(dr))):
                    act(halo(d, piece))

    each_halo(True, lambda copy: copy.start())
    for k in range(1, nx):
        pl.semaphore_signal(ready, inc=1, device_id=across(k), device_id_type=MESH)
    each_halo(False, lambda copy: copy.start())

    def shrink(x, start):
        sub = lax.broadcasted_iota(jnp.int32, (8, x.shape[1]), 0)
        ends = jnp.where(sub < 4, x[start + rows:start + rows + 8], x[start - 8:start])
        return jnp.concatenate([x[start:start + rows], ends], axis=0)

    def strip(a, begin, end):
        lane = lax.broadcasted_iota(jnp.int32, (end - begin, LANES), 1)
        edge = jnp.where(lane < half, right[a, begin:end], left[a, begin:end])
        return jnp.concatenate([main[a, begin:end], edge], axis=1)

    def field(a, window):
        if window == "tall":
            return strip(a, 0, tall)
        x = strip(a, low_mid, high_mid)
        return x if window == "mid" else shrink(x, 8)

    def up(x):
        return pltpu.roll(x, 1, 0)

    def down(x):
        return pltpu.roll(x, x.shape[0] - 1, 0)

    def before(x):
        return pltpu.roll(x, 1, 1)

    def after(x):
        return pltpu.roll(x, x.shape[1] - 1, 1)

    def masked(x, window):
        return jnp.where(scaled[window][...] > 0.0, x, 0.0)

    def core_of(window):
        return masked(SCALE * (field(1, window) + (inv_step + 4.0 - SHIFT)), window)

    def apply_b(v, core, window):
        beside = (up(v) + down(v)) + (before(v) + after(v))
        return core * v - scaled[window][...] * beside

    def apply_half(v, core):
        return (0.5 * core) * v - SCALE * (down(v) + after(v))

    def hamiltonian(u):
        dx = u - up(u)
        dy = u - before(u)
        px, qx = jnp.maximum(dx, 0.0), jnp.minimum(dx, 0.0)
        py, qy = jnp.maximum(dy, 0.0), jnp.minimum(dy, 0.0)
        return (px * px + down(qx * qx)) + (py * py + after(qy * qy))

    def faces(u):
        sx = u - down(u)
        sy = u - after(u)
        return jnp.maximum(sx, 0.0), jnp.minimum(sx, 0.0), jnp.maximum(sy, 0.0), jnp.minimum(sy, 0.0)

    def advance(m, face, window):
        px, qx, py, qy = face
        fx = px * m + qx * down(m)
        fy = py * m + qy * after(m)
        net = (fx - up(fx)) + (fy - before(fy))
        return scaled[window][...] * ((inv_step / SCALE) * m - (1.0 / SCALE) * net)

    def value_rhs(later, level, window):
        guess = masked(coupling * field(2 if level == 1 else 3, window), window)
        own_part = (inv_step / SCALE) * later - (0.5 / SCALE) * hamiltonian(later)
        return scaled[window][...] * own_part + guess

    def fold(p):
        parts = [p[i:i + 8, j:j + LANES] for i in range(0, rows, 8) for j in range(0, cols, LANES)]
        while len(parts) > 1:
            odd = parts[len(parts) // 2 * 2:]
            parts = [parts[i] + parts[i + 1] for i in range(0, len(parts) - 1, 2)] + odd
        return parts[0]

    def dot(x, y):
        return fold(x * y)

    sub8 = lax.broadcasted_iota(jnp.int32, (8, LANES), 0)
    lane8 = lax.broadcasted_iota(jnp.int32, (8, LANES), 1)

    def pack(tiles):
        spread = None
        for first in range(0, len(tiles), 8):
            group = tiles[first:first + 8]
            group = group + [jnp.zeros((8, LANES), jnp.float32)] * (8 - len(group))
            for step in (4, 2, 1):
                keep = lax.rem(sub8, 2 * step) < step
                group = [
                    jnp.where(keep, a + pltpu.roll(a, 8 - step, 0), b + pltpu.roll(b, step, 0))
                    for a, b in zip(group[:step], group[step:])
                ]
            sums = jnp.sum(group[0], axis=1, keepdims=True)
            part = jnp.where(lane8 == sub8 + first, sums, 0.0)
            spread = part if spread is None else spread + part
        return jnp.sum(spread, axis=0, keepdims=True)

    def send_sums(which, values):
        packed = pack(values)
        sent[which] = packed
        slots[which, me] = packed

        def send(px, py):
            pltpu.make_async_remote_copy(
                src_ref=sent.at[which], dst_ref=slots.at[which, me],
                send_sem=sum_send.at[which], recv_sem=sum_recv.at[which],
                device_id=(px, py), device_id_type=MESH).start()

        columns = [lax.rem(gy + k, ny) for k in range(ny)]

        def line(k, carry):
            px = lax.rem(gx + k, nx)
            for py in columns:
                send(px, py)
            return carry

        lax.fori_loop(1, nx, line, 0)
        for py in columns[1:]:
            send(gx, py)

    def take_sums(which, many):
        others = slots.at[which, pl.ds(0, count - 1)]
        pltpu.make_async_copy(others, others, sum_recv.at[which]).wait()
        total = jnp.sum(slots[which], axis=0)
        return [total[:, k:k + 1] for k in range(many)]

    def basis(b, core, window, last=True):
        v1 = apply_b(b, core, window)
        v2 = apply_b(v1, core, window)
        return (b, v1, v2, apply_half(v2, core)) if last else (b, v1, v2)

    def mix(c, v):
        return c[0] * v[0] + c[1] * v[1] + c[2] * v[2]

    def pairs(x, y):
        return [dot(x[0], y[0]), dot(x[0], y[1]), dot(x[1], y[1]),
                dot(x[1], y[2]), dot(x[2], y[2]),
                2.0 * dot(x[2], x[3]) if x is y
                else fold(x[2] * y[3] + y[2] * x[3])]

    def own_small(v):
        return [x[:rows, :cols] for x in v]

    each_halo(True, lambda copy: copy.wait_recv(), back=True)
    small_core = core_of("small")
    later = masked(field(0, "small"), "small")
    w = own_small(basis(value_rhs(later, 1, "small"), small_core, "small"))
    moments = pairs(w, w)
    pl.semaphore_wait(ready, nx - 1)
    send_sums(0, moments)
    each_halo(False, lambda copy: copy.wait_recv(), back=True)
    core = core_of("tall")
    later = masked(field(0, "tall"), "tall")
    v = basis(value_rhs(later, 1, "tall"), core, "tall", last=False)
    vs = [shrink(x, MARGIN) for x in v]
    c = solve_small(take_sums(0, 6))

    first_small = mix(c, vs)
    w = own_small(basis(value_rhs(first_small, 0, "small"), small_core, "small"))
    send_sums(1, pairs(w, w))
    first = mix(c, v)
    v = basis(value_rhs(first, 0, "tall"), core, "tall", last=False)
    v = [x[low_mid:high_mid] for x in v]
    face = faces(first_small)
    density = masked(field(4, "mid"), "mid")
    mid_core = core_of("mid")
    c = solve_small(take_sums(1, 6))
    second = mix(c, v)

    a = basis(advance(density, faces(second), "mid"), mid_core, "mid", last=False)
    a = [shrink(x, 8) for x in a]
    last = apply_half(a[2], small_core)
    inner = own_small(a + [last])
    families = [
        own_small(basis(advance(a[i], face, "small"), small_core, "small")) for i in range(3)]
    moments = pairs(inner, inner)
    for i in range(3):
        for j in range(i, 3):
            moments += pairs(families[i], families[j])
    send_sums(2, moments)
    both_ref[0] = second[8:8 + rows, :cols]
    each_halo(True, lambda copy: copy.wait_send())
    each_halo(False, lambda copy: copy.wait_send())
    for which in range(3):
        others = slots.at[which, pl.ds(0, count - 1)]
        pltpu.make_async_copy(others, others, sum_send.at[which]).wait()
    total = take_sums(2, len(moments))
    c = solve_small(total[:6])
    nu = [0.0] * 6
    at = 6
    for i in range(3):
        for j in range(i, 3):
            weight = c[i] * c[j] * (1.0 if i == j else 2.0)
            for k in range(6):
                nu[k] = nu[k] + weight * total[at + k]
            at += 6
    e = solve_small(nu)
    result = None
    for i in range(3):
        for k in range(3):
            part = (c[i] * e[k]) * families[i][k]
            result = part if result is None else result + part
    both_ref[1] = result


def solution(mesh):
    nx, ny = mesh.shape["gx"], mesh.shape["gy"]

    def shards(terminal, initial_density, density_guess, diagonal):
        rows, cols = terminal.shape
        tall = rows + 2 * MARGIN
        hbm = pl.BlockSpec(memory_space=pl.ANY)
        vmem = pl.BlockSpec(memory_space=pltpu.VMEM)
        shape = jax.ShapeDtypeStruct((rows, cols), jnp.float32)
        both = pl.pallas_call(
            functools.partial(kernel, nx, ny),
            out_shape=jax.ShapeDtypeStruct((2, rows, cols), jnp.float32),
            in_specs=[hbm] * 4,
            out_specs=vmem,
            scratch_shapes=[
                pltpu.VMEM((5, tall, cols), jnp.float32),
                pltpu.VMEM((5, tall, LANES), jnp.float32),
                pltpu.VMEM((5, tall, LANES), jnp.float32),
                pltpu.VMEM((3, 1, LANES), jnp.float32),
                pltpu.VMEM((3, nx * ny, 1, LANES), jnp.float32),
                pltpu.SemaphoreType.DMA((8, 3)),
                pltpu.SemaphoreType.DMA((8, 3)),
                pltpu.SemaphoreType.DMA((5,)),
                pltpu.SemaphoreType.DMA((3,)),
                pltpu.SemaphoreType.DMA((3,)),
                pltpu.SemaphoreType.REGULAR,
                pltpu.VMEM((tall, cols + LANES), jnp.float32),
                pltpu.VMEM((rows + 16, cols + LANES), jnp.float32),
                pltpu.VMEM((rows + 8, cols + LANES), jnp.float32),
            ],
            compiler_params=pltpu.CompilerParams(collective_id=0, has_side_effects=True),
        )(terminal, initial_density, density_guess, diagonal)
        return both[0], both[1]

    placed = (P("gx", "gy"), P("gx", "gy"), P(None, "gx", "gy"), P("gx", "gy"))
    return jax.shard_map(
        shards,
        mesh=mesh,
        in_specs=placed,
        out_specs=(P("gx", "gy"), P("gx", "gy")),
        check_vma=False,
    )
```
